256 devices in a mesh: vocab: 32 (over z, y), batch: 8 (over x, core).
Axes of the slice: x: 4, y: 4, z: 8, core: 2. Of those that a mesh axis runs over, the one named last changes fastest.
Arguments:
- latent_state_rows: bfloat16 [128, 8192], P('batch', 'vocab'), may hold values from -90 to 90
- closing_rescale_coeffs: bfloat16 [8192], replicated, may hold values from 0.5 to 1.5
- output_projection_matrix: bfloat16 [8192, 131072], P(None, ('vocab', 'batch')), may hold values from -3.7565048 to 3.7565048
- config_heat_values: float32 [16], replicated, may hold values from 0.7 to 1.4
- sequence_config_choice: int32 [128], replicated, may hold values from 0 to 15
- ranked_choice_ids: int32 [128, 128], replicated, may hold values from 0 to 131071
- keep_count: int32 [128], replicated, may hold values from 2 to 128
Outputs:
- log_norm: float32 [128], P('batch')
- kept_mass: float32 [128], P('batch')
- renormed: float32 [128, 128], P('batch')
The draws below stay inside these ranges and needn't reach their ends.
All inputs are finite; a program needn't handle non-finite values.
Results may differ from the reference program's by a relative error of at most 0.0048.
Values may be sent and summed in bfloat16 or wider, within the bound.
A program may use at most 64 MiB of HBM per device.

```python
import math
import jax
import jax.numpy as jnp
from jax import lax

D = 8192
VOCAB = 131072
CAND = 128
SAMPLER_CONFIGS = 16
SG = 16
SLOTS = 128
N_VOCAB = 32
N_BATCH = 8


def weight_block(key, block):
    return jnp.clip(jax.random.normal(jax.random.fold_in(jax.random.fold_in(key, 11), block), (D, 128), jnp.float32), -5.0, 5.0)


def column_scale(key):
    position = jnp.arange(VOCAB, dtype=jnp.float32) / VOCAB
    spread = jnp.exp(jax.random.uniform(jax.random.fold_in(key, 12), (VOCAB,), jnp.float32, math.log(0.45), math.log(2.2)))
    trend = 0.75 + 0.5 * position
    return 2.0 * spread * trend


def drawn_pairs():
    pairs = []
    targets = [160.0, 200.0, 240.0, 160.0, 200.0, 240.0]
    for number in range(6):
        first_id = (5003 + 24011 * number) % VOCAB
        second_id = (first_id + 7) % VOCAB
        row_index = number * SLOTS // 6
        pairs.append((first_id, second_id, row_index, targets[number]))
    return pairs


def draw_output_projection_matrix(key, part):
    blocks = jax.vmap(lambda block: weight_block(key, block), out_axes=1)(jnp.arange(VOCAB // 128))
    matrix = blocks.reshape(D, VOCAB) * (column_scale(key) / math.sqrt(D))[None, :]
    return matrix.astype(jnp.bfloat16)


def draw_latent_state_rows(key, part):
    values = jnp.clip(jax.random.normal(jax.random.fold_in(key, 13), (SLOTS, D), jnp.float32), -5.0, 5.0)
    return values.astype(jnp.bfloat16)


def draw_ranked_choice_ids(key, part):
    ids = jax.random.randint(jax.random.fold_in(key, 16), (SLOTS, CAND), 0, VOCAB, jnp.int32)
    shard_count = N_VOCAB * N_BATCH
    shard_width = VOCAB // shard_count
    group_of = jnp.arange(SLOTS, dtype=jnp.int32) // SG
    offsets = jax.random.randint(jax.random.fold_in(key, 17), (SLOTS, 2), 0, shard_width, jnp.int32)
    near_shard = (group_of + 1) % shard_count
    far_shard = (group_of + shard_count // 2) % shard_count
    ids = ids.at[:, 0].set(near_shard * shard_width + offsets[:, 0])
    ids = ids.at[:, 1].set(far_shard * shard_width + offsets[:, 1])
    for first_id, second_id, row_index, target in drawn_pairs():
        ids = ids.at[row_index, 0].set(jnp.int32(first_id))
        ids = ids.at[row_index, 1].set(jnp.int32(second_id))
    return ids


def touch_ends(values, own_key, low, top_value):
    extent = values.shape
    place = [jax.random.randint(jax.random.fold_in(own_key, axis), (), 0, extent[axis]) for axis in range(len(extent))]
    values = values.at[tuple(place)].set(low)
    longest = extent.index(max(extent))
    place[longest] = (place[longest] + 1) % extent[longest]
    return values.at[tuple(place)].set(top_value)


def setup_inputs(seed: int = 0) -> dict:
    key_list = jax.random.split(jax.random.key(seed), 8)
    latent_state_rows = draw_latent_state_rows(jax.random.fold_in(key_list[7], 71), 0)
    closing_rescale_coeffs = jnp.clip(1.0 + 0.1 * jax.random.normal(key_list[1], (D,), jnp.float32), 0.5, 1.5).astype(jnp.bfloat16)
    output_projection_matrix = draw_output_projection_matrix(jax.random.fold_in(key_list[7], 71), 0)
    config_heat_values = jnp.clip(jnp.exp(jax.random.uniform(key_list[3], (SAMPLER_CONFIGS,), jnp.float32, math.log(0.7), math.log(1.4))), 0.7, 1.4)
    sequence_config_choice = touch_ends(jax.random.randint(key_list[4], (SLOTS,), 0, SAMPLER_CONFIGS), jax.random.fold_in(key_list[4], 1), 0, SAMPLER_CONFIGS - 1).astype(jnp.int32)
    ranked_choice_ids = draw_ranked_choice_ids(jax.random.fold_in(key_list[7], 71), 0)
    keep_count = touch_ends(jax.random.randint(key_list[6], (SLOTS,), 2, CAND + 1), jax.random.fold_in(key_list[6], 1), 2, CAND).astype(jnp.int32)
    return {"latent_state_rows": latent_state_rows, "closing_rescale_coeffs": closing_rescale_coeffs, "output_projection_matrix": output_projection_matrix, "config_heat_values": config_heat_values, "sequence_config_choice": sequence_config_choice, "ranked_choice_ids": ranked_choice_ids, "keep_count": keep_count}


epsilon = 1e-06

def reference(latent_state_rows, closing_rescale_coeffs, output_projection_matrix, config_heat_values, sequence_config_choice, ranked_choice_ids, keep_count):
    values = latent_state_rows.astype(jnp.float32)
    mean_square = lax.optimization_barrier(jnp.mean(values * values, axis=1, keepdims=True))
    normed = (values * lax.rsqrt(mean_square + epsilon) * closing_rescale_coeffs.astype(jnp.float32)[None, :]).astype(jnp.bfloat16)
    unnormalized_scores = jnp.dot(normed, output_projection_matrix, preferred_element_type=jnp.float32)
    config_membership = (sequence_config_choice[:, None] == jnp.arange(SAMPLER_CONFIGS, dtype=jnp.int32)[None, :]).astype(jnp.float32)
    sequence_heat_values = lax.optimization_barrier(jnp.sum(config_membership * config_heat_values[None, :], axis=1))
    divided_scores = unnormalized_scores / sequence_heat_values[:, None]
    row_top = lax.optimization_barrier(jnp.max(divided_scores, axis=1))
    row_total = lax.optimization_barrier(jnp.sum(jnp.exp(divided_scores - row_top[:, None]), axis=1))
    log_norm = row_top + jnp.log(row_total)
    picked = jnp.take_along_axis(divided_scores, ranked_choice_ids.astype(jnp.int32), axis=1)
    kept_mask = jnp.arange(CAND, dtype=jnp.int32)[None, :] < keep_count[:, None]
    kept_top = lax.optimization_barrier(jnp.max(jnp.where(kept_mask, picked, jnp.float32(-3e+38)), axis=1))
    shifted = jnp.where(kept_mask, picked - kept_top[:, None], jnp.float32(0.0))
    kept_exp = jnp.where(kept_mask, jnp.exp(shifted), jnp.float32(0.0))
    kept_sum = lax.optimization_barrier(jnp.sum(kept_exp, axis=1))
    kept_mass = kept_top + jnp.log(kept_sum) - log_norm
    return (log_norm, kept_mass, kept_exp / kept_sum[:, None])
```

```python
import jax
import jax.numpy as jnp
from jax import lax
from jax.experimental import pallas as pl
from jax.experimental.pallas import tpu as pltpu
from jax.sharding import Mesh
from jax.sharding import PartitionSpec as P

NZ, NY, NX, NC = 8, 4, 4, 2
SG = 16
COLS = 512
LANES = 128
SLOTS = 128
D = 8192
EPS = 1e-06
MESH_ID = pl.DeviceIdType.MESH
ORDER = (0, 1, 7, 2, 6, 3, 5, 4)


def kernel(
    x_hbm, w_hbm, gain_hbm, ids_hbm, heat_ref, choice_hbm, keep_hbm,
    stat_out, ren_out,
    g_ref, w_ref, gain_ref, ids_ref, choice_ref, keep_ref,
    ssq_ref, acc_ref, m1_ref, r1_ref, r2_ref, r3_ref, m2_ref, m3_ref,
    in_sem, w_sem,
    s1_send, s1_recv, s2y_send, s2y_recv, s2x_send, s2x_recv,
    s3x_send, s3x_recv, s3y_send, s3y_recv,
    s4x_send, s4x_recv, s4y_send, s4y_recv, s5_send, s5_recv,
    q1_send, q1_recv, q2_send, q2_recv, q3_send, q3_recv,
):
    z0, y0, x0, c0 = (lax.axis_index(a) for a in ("z", "y", "x", "c"))

    def zp(k):
        return lax.rem(z0 + k, NZ)

    def yp(k):
        return lax.rem(y0 + k, NY)

    def xp(k):
        return lax.rem(x0 + k, NX)

    own = pltpu.make_async_copy(x_hbm, g_ref.at[z0, :, c0, x0, y0], in_sem.at[0])
    own.start()

    barrier = pltpu.get_barrier_semaphore()
    count = 0
    for k in range(1, NZ):
        pl.semaphore_signal(barrier, inc=1, device_id={"z": zp(k)}, device_id_type=MESH_ID)
        count += 1
    for k in range(1, NY):
        pl.semaphore_signal(barrier, inc=1, device_id={"y": yp(k)}, device_id_type=MESH_ID)
        count += 1
    for k in range(NX):
        for kc in range(NC):
            if k or kc:
                pl.semaphore_signal(
                    barrier, inc=1, device_id={"x": xp(k), "c": lax.rem(c0 + kc, NC)}, device_id_type=MESH_ID
                )
                count += 1

    w_copies = []
    for z in range(NZ):
        cp = pltpu.make_async_copy(w_hbm.at[z], w_ref.at[z], w_sem.at[z])
        cp.start()
        w_copies.append(cp)
    small = []
    for n, (src, dst) in enumerate(
        ((gain_hbm, gain_ref), (ids_hbm, ids_ref), (choice_hbm, choice_ref), (keep_hbm, keep_ref))
    ):
        cp = pltpu.make_async_copy(src, dst, in_sem.at[1 + n])
        cp.start()
        small.append(cp)
    own.wait()
    pl.semaphore_wait(barrier, count)

    sends = []

    def send(src, dst, ssem, rsem, to):
        cp = pltpu.make_async_remote_copy(
            src_ref=src, dst_ref=dst, send_sem=ssem, recv_sem=rsem, device_id=to, device_id_type=MESH_ID
        )
        cp.start()
        sends.append(cp)

    def landed(dst, ssem, rsem):
        pltpu.make_async_remote_copy(
            src_ref=dst, dst_ref=dst, send_sem=ssem, recv_sem=rsem, device_id={"z": z0}, device_id_type=MESH_ID
        ).wait_recv()

    for k in reversed(ORDER[1:]):
        blk = g_ref.at[z0, :, c0, x0, y0]
        send(blk, blk, s1_send.at[k], s1_recv.at[k], {"z": zp(k)})

    def stage2(k):
        z = zp(NZ - k)
        if k:
            landed(g_ref.at[z, :, c0, x0, y0], s1_send.at[k], s1_recv.at[k])
        for d in (2, 1, 3):
            a = g_ref.at[z, 0, c0, x0, y0]
            send(a, a, s2y_send.at[k, d], s2y_recv.at[k, d], {"y": yp(d)})
            b = g_ref.at[z, 1, c0, x0, y0]
            send(b, b, s2x_send.at[k, d], s2x_recv.at[k, d], {"x": xp(d)})

    def stage3(k):
        z = zp(NZ - k)
        for d in (1, 3, 2):
            landed(g_ref.at[z, 0, c0, x0, yp(NY - d)], s2y_send.at[k, d], s2y_recv.at[k, d])
        a = g_ref.at[z, 0, c0, x0]
        for d in (1, 3):
            send(a, a, s3x_send.at[k, d], s3x_recv.at[k, d], {"x": xp(d)})
        for d in (1, 3, 2):
            landed(g_ref.at[z, 1, c0, xp(NX - d), y0], s2x_send.at[k, d], s2x_recv.at[k, d])
        b = g_ref.at[z, 1, c0, :, y0]
        for d in (1, 3):
            send(b, b, s3y_send.at[k, d], s3y_recv.at[k, d], {"y": yp(d)})

    def stage4(k):
        z = zp(NZ - k)
        for d in (1, 3):
            part = pl.ds(0, 2) if d == 1 else pl.ds(2, 2)
            xs, ys = xp(NX - d), yp(NY - d)
            landed(g_ref.at[z, 0, c0, xs], s3x_send.at[k, d], s3x_recv.at[k, d])
            a = g_ref.at[z, 0, c0, xs, part]
            send(a, a, s4x_send.at[k, d], s4x_recv.at[k, d], {"x": xp(d)})
            landed(g_ref.at[z, 1, c0, :, ys], s3y_send.at[k, d], s3y_recv.at[k, d])
            b = g_ref.at[z, 1, c0, part, ys]
            send(b, b, s4y_send.at[k, d], s4y_recv.at[k, d], {"y": yp(d)})

    def stage5(k):
        z = zp(NZ - k)
        for d in (1, 3):
            part = pl.ds(0, 2) if d == 1 else pl.ds(2, 2)
            landed(g_ref.at[z, 0, c0, xp(2), part], s4x_send.at[k, d], s4x_recv.at[k, d])
            landed(g_ref.at[z, 1, c0, part, yp(2)], s4y_send.at[k, d], s4y_recv.at[k, d])
        blk = g_ref.at[z, :, c0]
        send(blk, blk, s5_send.at[k], s5_recv.at[k], {"c": lax.rem(c0 + 1, NC)})

    ssq_ref[...] = jnp.zeros_like(ssq_ref)

    def stage6(k):
        z = zp(NZ - k)
        landed(g_ref.at[z, :, lax.rem(c0 + 1, NC)], s5_send.at[k], s5_recv.at[k])
        total = ssq_ref[...]
        for h in range(2):
            for y in range(NY):
                v = g_ref[z, h, :, :, y].reshape(SLOTS, LANES).astype(jnp.float32)
                total += v * v
        ssq_ref[...] = total

    for stage, ks in (
        (stage2, (0, 1, 7)), (stage3, (0,)), (stage2, (2, 6, 3, 5, 4)),
        (stage3, (1, 7)), (stage4, (0,)), (stage3, (2, 6, 3, 5)), (stage4, (1, 7)),
        (stage5, (0,)), (stage3, (4,)), (stage4, (2, 6)), (stage6, (0,)), (stage4, (3, 5)),
        (stage5, (1, 7)), (stage4, (4,)), (stage5, (2, 6)), (stage6, (1, 7)), (stage5, (3, 5)),
        (stage6, (2, 6)), (stage5, (4,)), (stage6, (3, 5, 4)),
    ):
        for k in ks:
            stage(k)

    for cp in small:
        cp.wait()
    for cp in w_copies:
        cp.wait()

    mean_square = jnp.sum(ssq_ref[...], axis=1, keepdims=True) * (1.0 / D)
    factor = lax.rsqrt(mean_square + EPS)
    acc_ref[...] = jnp.zeros_like(acc_ref)

    @pl.loop(0, NZ * 2)
    def _(i):
        z, h = i // 2, lax.rem(i, 2)
        parts = []
        for y in range(NY):
            v = g_ref[z, h, :, :, y].reshape(SLOTS, LANES).astype(jnp.float32)
            gain = gain_ref[pl.ds(z * 8 + y * 2 + h, 1), :]
            parts.append((v * factor * gain).astype(jnp.bfloat16))
        lhs = jnp.concatenate(parts, axis=1)
        rhs = w_ref[z, :, h].reshape(NY * LANES, COLS)
        acc_ref[...] += jnp.dot(lhs, rhs, preferred_element_type=jnp.float32)

    lane = lax.broadcasted_iota(jnp.int32, (SLOTS, LANES), 1)
    row = lax.broadcasted_iota(jnp.int32, (SLOTS, LANES), 0)
    slot = (((row >> 4) & 3) * 2 + (row >> 6)) * SG + (row & 15)
    choice = choice_ref[...]
    heat = jnp.zeros((1, LANES), jnp.float32)
    for n in range(16):
        heat = jnp.where(choice == n, heat_ref[n], heat)
    heat = jnp.sum(jnp.where(lane == slot, heat, 0.0), axis=1, keepdims=True)
    scaled = acc_ref[...] / heat

    offset = ((z0 * NY + y0) * (NX * NC) + x0 * NC + c0) * COLS
    top = jnp.max(scaled, axis=1, keepdims=True)
    total = jnp.sum(jnp.exp(scaled - top), axis=1, keepdims=True)
    top_row = jnp.sum(jnp.where(lane == row, top, 0.0), axis=0, keepdims=True)
    total_row = jnp.sum(jnp.where(lane == row, total, 0.0), axis=0, keepdims=True)
    stats = jnp.concatenate([top_row, total_row, jnp.zeros((6, LANES), jnp.float32)], axis=0)
    for c in range(NC):
        for x in range(NX):
            g = c * NX + x
            mine = scaled[g * SG : (g + 1) * SG]
            local = ids_ref[x, c] - offset
            cand = jnp.zeros((SG, LANES), jnp.float32)
            for t in range(COLS // LANES):
                at = local - t * LANES
                inside = (at >= 0) & (at < LANES)
                got = jnp.take_along_axis(
                    mine[:, t * LANES : (t + 1) * LANES], jnp.clip(at, 0, LANES - 1), axis=1,
                    mode="promise_in_bounds",
                )
                cand = jnp.where(inside, got, cand)
            m1_ref[c, x, :SG] = cand
            m1_ref[c, x, SG:] = stats

    for k in (2, 1, 3, 0):
        for kc in range(NC):
            if k or kc:
                cx, cc = xp(k), lax.rem(c0 + kc, NC)
                send(
                    m1_ref.at[cc, cx], r1_ref.at[c0, x0],
                    q1_send.at[k, kc], q1_recv.at[k, kc], {"x": cx, "c": cc},
                )
    r1_ref[c0, x0] = m1_ref[c0, x0]
    for k in (0, 1, 3, 2):
        for kc in range(NC):
            if k or kc:
                landed(
                    r1_ref.at[lax.rem(c0 + kc, NC), xp(NX - k)], q1_send.at[k, kc], q1_recv.at[k, kc]
                )

    def merged(parts):
        top = parts[0][SG : SG + 1]
        for p in parts[1:]:
            top = jnp.maximum(top, p[SG : SG + 1])
        total, cand = jnp.zeros_like(top), jnp.zeros((SG, LANES), jnp.float32)
        for p in parts:
            total += p[SG + 1 : SG + 2] * jnp.exp(p[SG : SG + 1] - top)
            cand += p[:SG]
        return cand, top, total

    def store(ref, value):
        cand, top, total = value
        ref[:SG] = cand
        ref[SG:] = jnp.concatenate([top, total, jnp.zeros((6, LANES), jnp.float32)], axis=0)

    store(m2_ref, merged([r1_ref[c, x] for c in range(NC) for x in range(NX)]))
    for k in (2, 1, 3):
        send(m2_ref, r2_ref.at[y0], q2_send.at[k], q2_recv.at[k], {"y": yp(k)})
    r2_ref[y0] = m2_ref[...]
    for k in (1, 3, 2):
        landed(r2_ref.at[yp(NY - k)], q2_send.at[k], q2_recv.at[k])

    store(m3_ref, merged([r2_ref[y] for y in range(NY)]))
    for k in reversed(ORDER[1:]):
        send(m3_ref, r3_ref.at[z0], q3_send.at[k], q3_recv.at[k], {"z": zp(k)})
    r3_ref[z0] = m3_ref[...]
    for k in ORDER[1:]:
        landed(r3_ref.at[zp(NZ - k)], q3_send.at[k], q3_recv.at[k])
    cand, top, total = merged([r3_ref[z] for z in range(NZ)])

    log_norm = top + jnp.log(total)
    lane16 = lax.broadcasted_iota(jnp.int32, (SG, LANES), 1)
    row16 = lax.broadcasted_iota(jnp.int32, (SG, LANES), 0)
    at_row = lane16 == (c0 * NX + x0) * SG + row16
    log_norm = jnp.sum(jnp.where(at_row, log_norm, 0.0), axis=1, keepdims=True)
    at_slot = lane16 == (x0 * NC + c0) * SG + row16
    keep = jnp.sum(jnp.where(at_slot, keep_ref[...], 0), axis=1, keepdims=True)
    kept = lane16 < keep
    kept_top = jnp.max(jnp.where(kept, cand, -3e38), axis=1, keepdims=True)
    kept_exp = jnp.where(kept, jnp.exp(jnp.where(kept, cand - kept_top, 0.0)), 0.0)
    kept_sum = jnp.sum(kept_exp, axis=1, keepdims=True)
    kept_mass = kept_top + jnp.log(kept_sum) - log_norm
    ren_out[...] = kept_exp / kept_sum
    stat_out[0:1] = jnp.sum(jnp.where(lane16 == row16, log_norm, 0.0), axis=0, keepdims=True)
    stat_out[1:2] = jnp.sum(jnp.where(lane16 == row16, kept_mass, 0.0), axis=0, keepdims=True)
    stat_out[2:8] = jnp.zeros((6, LANES), jnp.float32)

    for cp in sends:
        cp.wait_send()


def local(x, gain, w, heat, choice, ids, keep):
    x = x.reshape(SG, 2, LANES).transpose(1, 0, 2)
    w = w.reshape(NZ, NY, 2, LANES, COLS)
    gain = gain.astype(jnp.float32).reshape(D // LANES, LANES)
    ids = ids.reshape(NX, NC, SG, LANES)
    any_spec = pl.BlockSpec(memory_space=pl.ANY)
    vmem = pl.BlockSpec(memory_space=pltpu.VMEM)
    dma = pltpu.SemaphoreType.DMA
    f32, bf16 = jnp.float32, jnp.bfloat16
    stats, ren = pl.pallas_call(
        kernel,
        name="tail",
        out_shape=(
            jax.ShapeDtypeStruct((8, LANES), f32),
            jax.ShapeDtypeStruct((SG, LANES), f32),
        ),
        in_specs=[any_spec] * 4 + [pl.BlockSpec(memory_space=pltpu.SMEM)] + [any_spec] * 2,
        out_specs=(vmem, vmem),
        scratch_shapes=[
            pltpu.VMEM((NZ, 2, NC, NX, NY, SG, LANES), bf16),
            pltpu.VMEM((NZ, NY, 2, LANES, COLS), bf16),
            pltpu.VMEM((D // LANES, LANES), f32),
            pltpu.VMEM((NX, NC, SG, LANES), jnp.int32),
            pltpu.VMEM((1, LANES), jnp.int32),
            pltpu.VMEM((1, LANES), jnp.int32),
            pltpu.VMEM((SLOTS, LANES), f32),
            pltpu.VMEM((SLOTS, COLS), f32),
            pltpu.VMEM((NC, NX, SG + 8, LANES), f32),
            pltpu.VMEM((NC, NX, SG + 8, LANES), f32),
            pltpu.VMEM((NY, SG + 8, LANES), f32),
            pltpu.VMEM((NZ, SG + 8, LANES), f32),
            pltpu.VMEM((SG + 8, LANES), f32),
            pltpu.VMEM((SG + 8, LANES), f32),
            dma((5,)), dma((NZ,)),
            dma((NZ,)), dma((NZ,)),
            dma((NZ, NY)), dma((NZ, NY)), dma((NZ, NX)), dma((NZ, NX)),
            dma((NZ, NX)), dma((NZ, NX)), dma((NZ, NY)), dma((NZ, NY)),
            dma((NZ, NX)), dma((NZ, NX)), dma((NZ, NY)), dma((NZ, NY)),
            dma((NZ,)), dma((NZ,)),
            dma((NX, NC)), dma((NX, NC)), dma((NY,)), dma((NY,)), dma((NZ,)), dma((NZ,)),
        ],
        compiler_params=pltpu.CompilerParams(
            collective_id=0, has_side_effects=True, vmem_limit_bytes=40 * 1024 * 1024
        ),
    )(x, w, gain, ids, heat, choice.reshape(1, SLOTS), keep.reshape(1, SLOTS))
    return stats[0, :SG], stats[1, :SG], ren


def solution(mesh):
    torus = Mesh(mesh.devices.reshape(NZ, NY, NX, NC), ("z", "y", "x", "c"))
    zy, xc = ("z", "y"), ("x", "c")
    in_specs = (P(xc, zy), P(), P(None, (*zy, *xc)), P(), P(), P(), P())
    out_specs = (P(xc), P(xc), P(xc, None))
    return jax.shard_map(local, mesh=torus, in_specs=in_specs, out_specs=out_specs, check_vma=False)
```

```python
import jax
import jax.numpy as jnp
from jax import lax
from jax.experimental import pallas as pl
from jax.experimental.pallas import tpu as pltpu
from jax.sharding import Mesh
from jax.sharding import PartitionSpec as P

NZ, NY, NX, NC = 8, 4, 4, 2
SG = 16
ROWS = SG + 2
COLS = 512
LANES = 128
SLOTS = 128
D = 8192
EPS = 1e-06
MESH_ID = pl.DeviceIdType.MESH


GROUPS = ((0, 1, 1), (1, 6, 2), (2, 4, 2), (3, 1, 3))
KIB_ROWS = 2


def offsets(g):
    first, stride, count = GROUPS[g]
    return [first + stride * n for n in range(count)]


def kernel(
    x_hbm, w_hbm, gain_hbm, ids_hbm, heat_hbm, choice_hbm, keep_hbm,
    out_ref,
    g_ref, w_ref, gain_ref, ids_ref, heat_ref, choice_ref, keep_ref,
    wide_ref, ssq_ref, acc_ref, m1_ref, r1_ref, r2_ref, r3_ref, m2_ref, m3_ref, size_ref,
    in_sem, w_sem, s1, s2, s3, s4, q_recv, ag_send, q_send,
):
    z0, y0, x0, c0 = (lax.axis_index(a) for a in ("z", "y", "x", "c"))

    def zp(k):
        return lax.rem(z0 + k, NZ)

    def yp(k):
        return lax.rem(y0 + k, NY)

    def xp(k):
        return lax.rem(x0 + k, NX)

    def cp_(k):
        return lax.rem(c0 + k, NC)

    for h in range(2):
        pltpu.make_async_copy(
            x_hbm.at[:, pl.ds(h * LANES, LANES)], g_ref.at[z0, h, c0, x0, y0], in_sem.at[0]
        ).start()

    peers = [{"z": zp(k)} for k in range(1, NZ)] + [{"y": yp(k)} for k in range(1, NY)]
    peers += [{"x": xp(k), "c": cp_(kc)} for k in range(NX) for kc in range(NC) if k or kc]
    barrier = pltpu.get_barrier_semaphore()
    for peer in peers:
        pl.semaphore_signal(barrier, inc=1, device_id=peer, device_id_type=MESH_ID)

    for z in range(NZ):
        pltpu.make_async_copy(w_hbm.at[z], w_ref.at[z], w_sem).start()
    small = []
    for n, (src, dst) in enumerate(
        (
            (gain_hbm, gain_ref), (ids_hbm, ids_ref), (heat_hbm, heat_ref),
            (choice_hbm, choice_ref), (keep_hbm, keep_ref),
        )
    ):
        cp = pltpu.make_async_copy(src, dst, in_sem.at[1 + n])
        cp.start()
        small.append(cp)
    own = g_ref.at[z0, :, c0, x0, y0]
    pltpu.make_async_copy(own, own, in_sem.at[0]).wait()
    pl.semaphore_wait(barrier, len(peers))

    sent = {}

    def send(src, dst, ssem, rsem, to, kib):
        pltpu.make_async_remote_copy(
            src_ref=src, dst_ref=dst, send_sem=ssem, recv_sem=rsem, device_id=to, device_id_type=MESH_ID
        ).start()
        sent[id(ssem)] = sent.get(id(ssem), 0) + kib

    def drain(sem, kib):
        whole = size_ref.at[pl.ds(0, kib * KIB_ROWS)]
        pltpu.make_async_copy(whole, whole, sem).wait()

    for g in reversed(range(1, len(GROUPS))):
        for k in offsets(g):
            send(own, own, ag_send, s1.at[g], {"z": zp(k)}, 8)

    def stage2(g):
        if g:
            drain(s1.at[g], 8 * GROUPS[g][2])
        for k in offsets(g):
            z = zp(NZ - k)
            for d in (2, 1, 3):
                a = g_ref.at[z, 0, c0, x0, y0]
                send(a, a, ag_send, s2.at[g], {"y": yp(d)}, 4)
                b = g_ref.at[z, 1, c0, x0, y0]
                send(b, b, ag_send, s2.at[g], {"x": xp(d)}, 4)

    def stage3(g):
        drain(s2.at[g], 24 * GROUPS[g][2])
        for k in offsets(g):
            z = zp(NZ - k)
            for d in (2, 1, 3):
                a = g_ref.at[z, 0, c0, x0]
                send(a, a, ag_send, s3.at[g], {"x": xp(d)}, 16)
                b = g_ref.at[z, 1, c0, :, y0]
                send(b, b, ag_send, s3.at[g], {"y": yp(d)}, 16)

    def stage4(g):
        drain(s3.at[g], 96 * GROUPS[g][2])
        for k in offsets(g):
            blk = g_ref.at[zp(NZ - k), :, c0]
            send(blk, blk, ag_send, s4.at[g], {"c": cp_(1)}, 128)

    def compute(g):
        if g == 0:
            for cp in small:
                cp.wait()
            pltpu.make_async_copy(w_ref, w_ref, w_sem).wait()
            wide_ref[...] = gain_ref[...].astype(jnp.float32)
            ssq_ref[...] = jnp.zeros_like(ssq_ref)
            acc_ref[...] = jnp.zeros_like(acc_ref)
        drain(s4.at[g], 128 * GROUPS[g][2])
        first, stride, count = GROUPS[g]

        def chunk(n):
            z = lax.rem(z0 + (NZ - first) + (NZ - stride) * n, NZ)
            high, low = [], []
            total = ssq_ref[...]
            for y in range(NY):
                for h in range(2):
                    v = g_ref[z, h, :, :, y].reshape(SLOTS, LANES).astype(jnp.float32)
                    total += v * v
                    p = v * wide_ref[pl.ds(z * 8 + y * 2 + h, 1), :]
                    hi = p.astype(jnp.bfloat16)
                    high.append(hi)
                    low.append((p - hi.astype(jnp.float32)).astype(jnp.bfloat16))
            ssq_ref[...] = total
            lhs = jnp.concatenate([jnp.concatenate(high, axis=1), jnp.concatenate(low, axis=1)], axis=0)
            rhs = w_ref[z].reshape(2 * NY * LANES, COLS)
            both = jnp.dot(lhs, rhs, preferred_element_type=jnp.float32)
            acc_ref[...] += both[:SLOTS] + both[SLOTS:]

        if count == 1:
            chunk(0)
        else:
            pl.loop(0, count)(chunk)

    stage2(0)
    stage2(1)
    stage2(2)
    stage3(0)
    stage2(3)
    stage3(1)
    stage3(2)
    stage4(0)
    stage3(3)
    compute(0)
    stage4(1)
    stage4(2)
    compute(1)
    stage4(3)
    compute(2)
    compute(3)

    mean_square = jnp.sum(ssq_ref[...], axis=1, keepdims=True) * (1.0 / D)
    factor = lax.rsqrt(mean_square + EPS)

    lane = lax.broadcasted_iota(jnp.int32, (SLOTS, LANES), 1)
    row = lax.broadcasted_iota(jnp.int32, (SLOTS, LANES), 0)
    slot = (((row >> 4) & 3) * 2 + (row >> 6)) * SG + (row & 15)
    choice = choice_ref[...]
    heat = jnp.zeros((1, LANES), jnp.float32)
    for n in range(16):
        heat = jnp.where(choice == n, heat_ref[n], heat)
    heat = jnp.sum(jnp.where(lane == slot, heat, 0.0), axis=1, keepdims=True)
    scaled = acc_ref[...] * (factor / heat)

    offset = ((z0 * NY + y0) * (NX * NC) + x0 * NC + c0) * COLS
    top = jnp.max(scaled, axis=1, keepdims=True)
    total = jnp.sum(jnp.exp(scaled - top), axis=1, keepdims=True)
    top_row = jnp.sum(jnp.where(lane == row, top, 0.0), axis=0, keepdims=True)
    total_row = jnp.sum(jnp.where(lane == row, total, 0.0), axis=0, keepdims=True)
    stats = jnp.concatenate([top_row, total_row], axis=0)
    for c in range(NC):
        for x in range(NX):
            g = c * NX + x
            mine = scaled[g * SG : (g + 1) * SG]
            local = ids_ref[x, c] - offset
            cand = jnp.zeros((SG, LANES), jnp.float32)
            for t in range(COLS // LANES):
                at = local - t * LANES
                inside = (at >= 0) & (at < LANES)
                got = jnp.take_along_axis(
                    mine[:, t * LANES : (t + 1) * LANES], jnp.clip(at, 0, LANES - 1), axis=1,
                    mode="promise_in_bounds",
                )
                cand = jnp.where(inside, got, cand)
            m1_ref[c, x, :SG] = cand
            m1_ref[c, x, SG:ROWS] = stats

    part = pl.ds(0, ROWS)
    for k in (2, 1, 3, 0):
        for kc in range(NC):
            if k or kc:
                cx, cc = xp(k), cp_(kc)
                send(
                    m1_ref.at[cc, cx, part], r1_ref.at[c0, x0, part],
                    q_send, q_recv.at[0], {"x": cx, "c": cc}, 9,
                )
    r1_ref[c0, x0, :ROWS] = m1_ref[c0, x0, :ROWS]
    drain(q_recv.at[0], 7 * 9)

    def merged(parts):
        top = parts[0][SG : SG + 1]
        for p in parts[1:]:
            top = jnp.maximum(top, p[SG : SG + 1])
        total, cand = jnp.zeros_like(top), jnp.zeros((SG, LANES), jnp.float32)
        for p in parts:
            total += p[SG + 1 : SG + 2] * jnp.exp(p[SG : SG + 1] - top)
            cand += p[:SG]
        return cand, top, total

    def store(ref, value):
        cand, top, total = value
        ref[:SG] = cand
        ref[SG:ROWS] = jnp.concatenate([top, total], axis=0)

    store(m2_ref, merged([r1_ref[c, x, :ROWS] for c in range(NC) for x in range(NX)]))
    for k in (2, 1, 3):
        send(m2_ref.at[part], r2_ref.at[y0, part], q_send, q_recv.at[1], {"y": yp(k)}, 9)
    r2_ref[y0, :ROWS] = m2_ref[:ROWS]
    drain(q_recv.at[1], 3 * 9)

    store(m3_ref, merged([r2_ref[y, :ROWS] for y in range(NY)]))
    for k in (4, 3, 5, 2, 6, 1, 7):
        send(m3_ref.at[part], r3_ref.at[z0, part], q_send, q_recv.at[2], {"z": zp(k)}, 9)
    r3_ref[z0, :ROWS] = m3_ref[:ROWS]
    drain(q_recv.at[2], 7 * 9)
    cand, top, total = merged([r3_ref[z, :ROWS] for z in range(NZ)])

    log_norm = top + jnp.log(total)
    lane16 = lax.broadcasted_iota(jnp.int32, (SG, LANES), 1)
    row16 = lax.broadcasted_iota(jnp.int32, (SG, LANES), 0)
    at_row = lane16 == (c0 * NX + x0) * SG + row16
    log_norm = jnp.sum(jnp.where(at_row, log_norm, 0.0), axis=1, keepdims=True)
    at_slot = lane16 == (x0 * NC + c0) * SG + row16
    keep = jnp.sum(jnp.where(at_slot, keep_ref[...], 0), axis=1, keepdims=True)
    kept = lane16 < keep
    kept_top = jnp.max(jnp.where(kept, cand, -3e38), axis=1, keepdims=True)
    kept_exp = jnp.where(kept, jnp.exp(jnp.where(kept, cand - kept_top, 0.0)), 0.0)
    kept_sum = jnp.sum(kept_exp, axis=1, keepdims=True)
    kept_mass = kept_top + jnp.log(kept_sum) - log_norm
    out_ref[8:] = kept_exp / kept_sum
    out_ref[0:1] = jnp.sum(jnp.where(lane16 == row16, log_norm, 0.0), axis=0, keepdims=True)
    out_ref[1:2] = jnp.sum(jnp.where(lane16 == row16, kept_mass, 0.0), axis=0, keepdims=True)
    out_ref[2:8] = jnp.zeros((6, LANES), jnp.float32)

    drain(ag_send, sent[id(ag_send)])
    drain(q_send, sent[id(q_send)])


def local(x, gain, w, heat, choice, ids, keep):
    w = w.reshape(NZ, NY, 2, LANES, COLS)
    gain = gain.reshape(D // LANES, LANES)
    ids = ids.reshape(NX, NC, SG, LANES)
    hbm = pl.BlockSpec(memory_space=pl.ANY)
    vmem = pl.BlockSpec(memory_space=pltpu.VMEM)
    operands = (x, w, gain, ids, heat, choice.reshape(1, SLOTS), keep.reshape(1, SLOTS))
    dma = pltpu.SemaphoreType.DMA
    f32, bf16 = jnp.float32, jnp.bfloat16
    out = pl.pallas_call(
        kernel,
        name="tail",
        out_shape=jax.ShapeDtypeStruct((8 + SG, LANES), f32),
        in_specs=[hbm] * 7,
        out_specs=vmem,
        scratch_shapes=[
            pltpu.VMEM((NZ, 2, NC, NX, NY, SG, LANES), bf16),
            pltpu.VMEM((NZ, NY, 2, LANES, COLS), bf16),
            pltpu.VMEM((D // LANES, LANES), bf16),
            pltpu.VMEM((NX, NC, SG, LANES), jnp.int32),
            pltpu.SMEM((16,), f32),
            pltpu.VMEM((1, LANES), jnp.int32),
            pltpu.VMEM((1, LANES), jnp.int32),
            pltpu.VMEM((D // LANES, LANES), f32),
            pltpu.VMEM((SLOTS, LANES), f32),
            pltpu.VMEM((SLOTS, COLS), f32),
            pltpu.VMEM((NC, NX, SG + 8, LANES), f32),
            pltpu.VMEM((NC, NX, SG + 8, LANES), f32),
            pltpu.VMEM((NY, SG + 8, LANES), f32),
            pltpu.VMEM((NZ, SG + 8, LANES), f32),
            pltpu.VMEM((SG + 8, LANES), f32),
            pltpu.VMEM((SG + 8, LANES), f32),
            pltpu.VMEM((4096, LANES), f32),
            dma((6,)), dma, dma((4,)), dma((4,)), dma((4,)), dma((4,)), dma((3,)), dma, dma,
        ],
        compiler_params=pltpu.CompilerParams(
            collective_id=0, has_side_effects=True, vmem_limit_bytes=32 * 1024 * 1024
        ),
    )(*(pltpu.with_memory_space_constraint(a, pltpu.HBM) for a in operands))
    return out[0, :SG], out[1, :SG], out[8:]


def solution(mesh):
    torus = Mesh(mesh.devices.reshape(NZ, NY, NX, NC), ("z", "y", "x", "c"))
    zy, xc = ("z", "y"), ("x", "c")
    in_specs = (P(xc, zy), P(), P(None, (*zy, *xc)), P(), P(), P(), P())
    out_specs = (P(xc), P(xc), P(xc, None))
    return jax.shard_map(local, mesh=torus, in_specs=in_specs, out_specs=out_specs, check_vma=False)
```
